32 devices in a mesh: groups: 2 (over y), ctx: 16 (over z, x, core).
Axes of the slice: x: 2, y: 2, z: 4, core: 2. Of those that a mesh axis runs over, the one named last changes fastest.
Arguments:
- query_rows: bfloat16 [4096, 2560], P(('groups', 'ctx')), parts along dimension 0, may hold values from -211 to 211
- key_rows: bfloat16 [4096, 2560], P(('groups', 'ctx')), parts along dimension 0, may hold values from -6.2 to 6.2
- value_rows: bfloat16 [4096, 2560], P(('groups', 'ctx')), parts along dimension 0, may hold values from -6 to 6
- out_grad: bfloat16 [4096, 2560], P(('groups', 'ctx')), parts along dimension 0, may hold values from -6 to 6
- selected: int32 [32, 8], P('groups'), parts along dimension 0, may hold values from 0 to 15, as said below
Outputs:
- attended: bfloat16 [4096, 2560], P(('groups', 'ctx')), parts along dimension 0
- grad_query: bfloat16 [4096, 2560], P(('groups', 'ctx')), parts along dimension 0
- grad_key: bfloat16 [4096, 2560], P(('groups', 'ctx')), parts along dimension 0
- grad_value: bfloat16 [4096, 2560], P(('groups', 'ctx')), parts along dimension 0
- pooled_key_grad: float32 [64, 2560], P(('groups', 'ctx')), parts along dimension 0
- pooled_value_grad: float32 [64, 2560], P(('groups', 'ctx')), parts along dimension 0
The draws below stay inside these ranges and needn't reach their ends.
There are 2 independent parts, one for each index of `groups`. The reference program is written for one: setup_inputs(seed, part) draws one part's arguments, and reference() takes and returns one part's arrays. A program takes and returns all parts, laid end to end along the dimension named above; each array names one. Nothing has to cross between parts.
Inputs may be any that keep to these rules, and one draw needn't show every extreme that they name: `selected`: each row names 8 different tiles.
All inputs are finite; a program needn't handle non-finite values.
Results may differ from the reference program's by a relative error of at most 0.029.
Values may be sent and summed in bfloat16 or wider, within the bound.
A program may use at most 192 MiB of HBM per device.

```python
import jax
import jax.numpy as jnp
from jax import lax

HEADS = 20
HEAD_DIM = 128
TILE = 128
POOL = 64
SEL = 8
TILES = 16
TOKENS = 2048
COMP = 32


def draw_selected(key, part):
    seeded = jax.random.fold_in(key, 101)
    popular = jax.random.randint(jax.random.fold_in(seeded, 1), (TILES,), 0, 4)
    jitter = jax.random.randint(jax.random.fold_in(seeded, 2), (TILES, TILES), 0, 4096)
    tile_ids = jnp.arange(TILES, dtype=jnp.int32)
    order = jax.random.permutation(jax.random.fold_in(seeded, 3), TILES).astype(jnp.int32)
    place = jnp.zeros((TILES,), jnp.int32).at[order].set(tile_ids)
    offset = (place[None, :] - tile_ids[:, None]) % TILES
    base = (offset < SEL // 2).astype(jnp.int32)
    ranking = (jitter + 1024 * popular[None, :] + 16384 * base) * TILES + tile_ids[None, :]
    return lax.top_k(ranking, SEL)[1].astype(jnp.int32)


def block_rows(key, stamp):
    columns = HEADS * HEAD_DIM
    common = jax.random.normal(jax.random.fold_in(key, stamp), (COMP, 1, columns), jnp.float32)
    jitter = jax.random.normal(jax.random.fold_in(key, stamp + 1), (COMP, POOL, columns), jnp.float32)
    return jnp.clip((common + jitter) * 0.7071, -6.0, 6.0).reshape(TOKENS, columns)


def draw_key_rows(key, part):
    result = block_rows(key, 201)
    return jnp.clip(result, -6.2, 6.2).astype(jnp.bfloat16)


def draw_query_rows(key, part):
    columns = HEADS * HEAD_DIM
    result = jnp.clip(1.5 * jax.random.normal(jax.random.fold_in(key, 401), (TOKENS, columns), jnp.float32), -8.0, 8.0)
    return result.astype(jnp.bfloat16)


def draw_value_rows(key, part):
    return block_rows(key, 301).astype(jnp.bfloat16)


def draw_out_grad(key, part):
    columns = HEADS * HEAD_DIM
    result = jax.random.normal(jax.random.fold_in(key, 502), (TOKENS, columns), jnp.float32)
    return jnp.clip(result, -6.0, 6.0).astype(jnp.bfloat16)


def setup_inputs(seed: int = 0, part: int = 0) -> dict:
    key_list = jax.random.split(jax.random.key(seed), 6)
    part_splits = jax.random.split(jax.random.fold_in(key_list[5], part), 6)
    return {
        "query_rows": draw_query_rows(jax.random.fold_in(jax.random.fold_in(key_list[5], part), 71), part),
        "key_rows": draw_key_rows(jax.random.fold_in(jax.random.fold_in(key_list[5], part), 71), part),
        "value_rows": draw_value_rows(jax.random.fold_in(jax.random.fold_in(key_list[5], part), 71), part),
        "out_grad": draw_out_grad(jax.random.fold_in(jax.random.fold_in(key_list[5], part), 71), part),
        "selected": draw_selected(jax.random.fold_in(jax.random.fold_in(key_list[5], part), 71), part),
    }


def pooled(rows):
    return jnp.mean(rows.astype(jnp.float32).reshape(-1, POOL, rows.shape[1]), axis=1).astype(jnp.bfloat16)


def settle(array):
    return lax.optimization_barrier(array.astype(jnp.bfloat16)).astype(jnp.float32)


def tile_pass(queries, grads_out, keys_all, values_all):
    scaling = HEAD_DIM ** -0.5
    height = queries.shape[0]
    key_count = keys_all.shape[0]
    columns = HEADS * HEAD_DIM
    highest = lax.Precision.HIGHEST
    head_query = queries.astype(jnp.float32).reshape(height, HEADS, HEAD_DIM)
    head_grad = grads_out.astype(jnp.float32).reshape(height, HEADS, HEAD_DIM)
    head_key = keys_all.astype(jnp.float32).reshape(key_count, HEADS, HEAD_DIM)
    head_value = values_all.astype(jnp.float32).reshape(key_count, HEADS, HEAD_DIM)
    scores = jnp.einsum("rhd,khd->hrk", head_query, head_key, precision=highest) * scaling
    summit = jnp.max(scores, axis=-1, keepdims=True)
    raised = jnp.exp(scores - summit)
    weights = raised / jnp.sum(raised, axis=-1, keepdims=True)
    rounded = settle(weights)
    attended = jnp.einsum("hrk,khd->rhd", rounded, head_value, precision=highest).astype(jnp.bfloat16)
    row_dots = jnp.sum(head_grad * attended.astype(jnp.float32), axis=-1)
    prob_grad = jnp.einsum("rhd,khd->hrk", head_grad, head_value, precision=highest)
    score_grad = settle(weights * (prob_grad - row_dots.T[:, :, None]))
    grad_query = (jnp.einsum("hrk,khd->rhd", score_grad, head_key, precision=highest) * scaling).astype(jnp.bfloat16)
    key_terms = jnp.einsum("hrk,rhd->khd", score_grad, head_query, precision=highest) * scaling
    value_terms = jnp.einsum("hrk,rhd->khd", rounded, head_grad, precision=highest)
    return (attended.reshape(height, columns), grad_query.reshape(height, columns),
            key_terms.reshape(key_count, columns), value_terms.reshape(key_count, columns))


def reference(query_rows, key_rows, value_rows, out_grad, selected):
    columns = HEADS * HEAD_DIM
    pool_keys = pooled(key_rows)
    pool_values = pooled(value_rows)
    key_tiles = key_rows.reshape(TILES, TILE, columns)
    value_tiles = value_rows.reshape(TILES, TILE, columns)

    def advance(totals, inputs):
        coarse_keys, coarse_values, fine_keys, fine_values = totals
        queries, grads_out, listed = inputs
        keys_all = jnp.concatenate([pool_keys, key_tiles[listed].reshape(SEL * TILE, columns)], axis=0)
        values_all = jnp.concatenate([pool_values, value_tiles[listed].reshape(SEL * TILE, columns)], axis=0)
        attended, grad_query, key_terms, value_terms = tile_pass(queries, grads_out, keys_all, values_all)
        coarse_keys = coarse_keys + key_terms[:COMP]
        coarse_values = coarse_values + value_terms[:COMP]
        fine_keys = fine_keys.at[listed].add(settle(key_terms[COMP:]).reshape(SEL, TILE, columns))
        fine_values = fine_values.at[listed].add(settle(value_terms[COMP:]).reshape(SEL, TILE, columns))
        return (coarse_keys, coarse_values, fine_keys, fine_values), (attended, grad_query)

    initial = (jnp.zeros((COMP, columns), jnp.float32), jnp.zeros((COMP, columns), jnp.float32),
               jnp.zeros((TILES, TILE, columns), jnp.float32), jnp.zeros((TILES, TILE, columns), jnp.float32))
    totals, outputs = lax.scan(advance, initial, (query_rows.reshape(TILES, TILE, columns),
                                                  out_grad.reshape(TILES, TILE, columns), selected))
    coarse_keys, coarse_values, fine_keys, fine_values = totals
    attended = outputs[0].reshape(TOKENS, columns)
    grad_query = outputs[1].reshape(TOKENS, columns)
    grad_key = (settle(fine_keys.reshape(TOKENS, columns)) + jnp.repeat(coarse_keys, POOL, axis=0) / POOL).astype(jnp.bfloat16)
    grad_value = (settle(fine_values.reshape(TOKENS, columns)) + jnp.repeat(coarse_values, POOL, axis=0) / POOL).astype(jnp.bfloat16)
    return (attended, grad_query, grad_key, grad_value, coarse_keys, coarse_values)
```

```python
import jax
import jax.numpy as jnp
from jax import lax
from jax.experimental import pallas as pl
from jax.experimental.pallas import tpu as pltpu
from jax.sharding import PartitionSpec as P

HEADS = 20
HEAD_DIM = 128
TILE = 128
POOL = 64
SEL = 8
CHUNKS = 4
CORES = 2
PAIR = 2


def pooled(rows):
    return jnp.mean(rows.astype(jnp.float32).reshape(-1, POOL, rows.shape[1]), axis=1).astype(
        jnp.bfloat16
    )


def contract(left, right, left_dim, right_dim):
    return lax.dot_general(
        left, right, (((left_dim,), (right_dim,)), ((), ())), preferred_element_type=jnp.float32
    )


def attend(queries, grads_out, keys_all, values_all):
    scaling = HEAD_DIM ** (-0.5)
    out_parts, query_parts, key_parts, value_parts = ([], [], [], [])
    for head in range(HEADS):
        lower = head * HEAD_DIM
        upper = lower + HEAD_DIM
        head_query = queries[:, lower:upper]
        head_grad = grads_out[:, lower:upper]
        head_key = keys_all[:, lower:upper]
        head_value = values_all[:, lower:upper]
        scores = contract(head_query, head_key, 1, 1) * scaling
        summit = jnp.max(scores, axis=-1, keepdims=True)
        raised = jnp.exp(scores - summit)
        weights = raised / jnp.sum(raised, axis=-1, keepdims=True)
        rounded = weights.astype(jnp.bfloat16)
        out_rows = jnp.dot(rounded, head_value, preferred_element_type=jnp.float32).astype(
            jnp.bfloat16
        )
        row_dots = jnp.sum(
            head_grad.astype(jnp.float32) * out_rows.astype(jnp.float32), axis=-1, keepdims=True
        )
        prob_grad = contract(head_grad, head_value, 1, 1)
        score_grad = (weights * (prob_grad - row_dots)).astype(jnp.bfloat16)
        query_grad = jnp.dot(score_grad, head_key, preferred_element_type=jnp.float32) * scaling
        key_terms = contract(score_grad, head_query, 0, 0) * scaling
        value_terms = contract(rounded, head_grad, 0, 0)
        out_parts.append(out_rows)
        query_parts.append(query_grad.astype(jnp.bfloat16))
        key_parts.append(key_terms)
        value_parts.append(value_terms)
    return (
        jnp.concatenate(out_parts, axis=1),
        jnp.concatenate(query_parts, axis=1),
        jnp.concatenate(key_parts, axis=1),
        jnp.concatenate(value_parts, axis=1),
    )


def package(tiles_in, pooled_in, devices, spread):
    tiles_here, tile_len, columns = tiles_in.shape
    per_tile = tile_len // POOL
    split_rows = tiles_in.reshape(tiles_here, devices, spread, columns)
    copies = jnp.broadcast_to(
        pooled_in.reshape(tiles_here, 1, per_tile, columns),
        (tiles_here, devices, per_tile, columns),
    )
    return jnp.concatenate([split_rows, copies], axis=2).reshape(
        tiles_here, devices * (spread + per_tile), columns
    )


def listed_shards(query_rows, key_rows, value_rows, out_grad, selected):
    height, columns = query_rows.shape
    devices = lax.axis_size("ctx")
    tiles_here = height // TILE
    spread = TILE // devices
    own_keys = pooled(key_rows)
    own_values = pooled(value_rows)
    key_tiles = key_rows.reshape(tiles_here, TILE, columns)
    value_tiles = value_rows.reshape(tiles_here, TILE, columns)
    joined_keys, joined_values = (
        lax.all_to_all(
            package(key_tiles, own_keys, devices, spread),
            "ctx",
            split_axis=1,
            concat_axis=0,
            tiled=True,
        ),
        lax.all_to_all(
            package(value_tiles, own_values, devices, spread),
            "ctx",
            split_axis=1,
            concat_axis=0,
            tiled=True,
        ),
    )
    held_keys = joined_keys[:, :spread]
    held_values = joined_values[:, :spread]
    pool_keys = joined_keys[:, spread:].reshape(-1, columns)
    pool_values = joined_values[:, spread:].reshape(-1, columns)
    comp_count = pool_keys.shape[0]
    got_keys, got_values = (
        lax.all_to_all(held_keys[selected], "ctx", split_axis=0, concat_axis=2, tiled=True),
        lax.all_to_all(held_values[selected], "ctx", split_axis=0, concat_axis=2, tiled=True),
    )
    fine_keys = got_keys.reshape(tiles_here, SEL * TILE, columns)
    fine_values = got_values.reshape(tiles_here, SEL * TILE, columns)
    out_tiles, query_tiles, key_listed, value_listed = ([], [], [], [])
    keys_all = jnp.concatenate([pool_keys, fine_keys[0]], axis=0)
    values_all = jnp.concatenate([pool_values, fine_values[0]], axis=0)
    out_rows, query_grad, key_terms, value_terms = attend(
        query_rows, out_grad, keys_all, values_all
    )
    out_tiles.append(out_rows)
    query_tiles.append(query_grad)
    coarse_keys = key_terms[:comp_count]
    coarse_values = value_terms[:comp_count]
    key_listed.append(key_terms[comp_count:].astype(jnp.bfloat16))
    value_listed.append(value_terms[comp_count:].astype(jnp.bfloat16))
    own_coarse_keys, own_coarse_values = (
        lax.psum_scatter(coarse_keys, "ctx", scatter_dimension=0, tiled=True),
        lax.psum_scatter(coarse_values, "ctx", scatter_dimension=0, tiled=True),
    )
    listed_keys = jnp.stack(key_listed).reshape(tiles_here * SEL, devices, spread, columns)
    listed_values = jnp.stack(value_listed).reshape(tiles_here * SEL, devices, spread, columns)
    back_keys, back_values = (
        lax.all_to_all(listed_keys, "ctx", split_axis=1, concat_axis=0, tiled=True),
        lax.all_to_all(listed_values, "ctx", split_axis=1, concat_axis=0, tiled=True),
    )
    tile_ids = jnp.arange(selected.shape[0], dtype=jnp.int32)[:, None]
    member = (selected.reshape(1, -1) == tile_ids).astype(jnp.bfloat16)
    entries = member.shape[1]
    sum_keys = jnp.dot(
        member, back_keys.reshape(entries, spread * columns), preferred_element_type=jnp.float32
    )
    sum_values = jnp.dot(
        member, back_values.reshape(entries, spread * columns), preferred_element_type=jnp.float32
    )
    held_key_grad = sum_keys.astype(jnp.bfloat16).reshape(devices, tiles_here, spread, columns)
    held_value_grad = sum_values.astype(jnp.bfloat16).reshape(devices, tiles_here, spread, columns)
    owned_keys, owned_values = (
        lax.all_to_all(held_key_grad, "ctx", split_axis=0, concat_axis=2, tiled=True),
        lax.all_to_all(held_value_grad, "ctx", split_axis=0, concat_axis=2, tiled=True),
    )
    grad_key = (
        owned_keys.reshape(height, columns).astype(jnp.float32)
        + jnp.repeat(own_coarse_keys, POOL, axis=0) / POOL
    ).astype(jnp.bfloat16)
    grad_value = (
        owned_values.reshape(height, columns).astype(jnp.float32)
        + jnp.repeat(own_coarse_values, POOL, axis=0) / POOL
    ).astype(jnp.bfloat16)
    attended = out_tiles[0]
    grad_query = query_tiles[0]
    return (attended, grad_query, grad_key, grad_value, own_coarse_keys, own_coarse_values)


def head_kernel(place_ref, query_ref, grad_ref, near_ref, far_ref, mean_ref, out_ref, dq_ref,
                dnear_ref, dfar_ref, coarse_ref, keys, values):
    half = near_ref.shape[0] // TILE
    fine = SEL * TILE
    count = keys.shape[0]
    means = (
        jnp.dot(mean_ref[:, : half * TILE], near_ref[...], preferred_element_type=jnp.float32)
        + jnp.dot(mean_ref[:, half * TILE :], far_ref[...], preferred_element_type=jnp.float32)
    ) * (1.0 / POOL)
    keys[fine:, :] = means[:, :HEAD_DIM].astype(jnp.bfloat16)
    values[fine:, :] = means[:, HEAD_DIM:].astype(jnp.bfloat16)
    dnear_ref[...] = jnp.zeros_like(dnear_ref)
    dfar_ref[...] = jnp.zeros_like(dfar_ref)
    for j in range(SEL):
        place = place_ref[j]
        rows = slice(j * TILE, (j + 1) * TILE)
        for side, ref in enumerate((near_ref, far_ref)):
            start = pl.multiple_of((place % half) * TILE, TILE)

            @pl.when(place // half == side)
            def _():
                keys[rows, :] = ref[pl.ds(start, TILE), :HEAD_DIM]
                values[rows, :] = ref[pl.ds(start, TILE), HEAD_DIM:]

    scaling = HEAD_DIM ** (-0.5)
    query = query_ref[...]
    grad = grad_ref[...]
    all_keys = keys[...]
    all_values = values[...]
    scores = contract(all_keys, query, 1, 1)
    summit = jnp.max(scores, axis=0, keepdims=True)
    raised = jnp.exp((scores - summit) * scaling)
    weights = raised * (1.0 / jnp.sum(raised, axis=0, keepdims=True))
    rounded = weights.astype(jnp.bfloat16)
    out_rows = contract(rounded, all_values, 0, 0).astype(jnp.bfloat16)
    out_ref[...] = out_rows
    products = grad.astype(jnp.float32) * out_rows.astype(jnp.float32)
    row_dots = jnp.sum(products.T, axis=0, keepdims=True)
    prob_grad = contract(all_values, grad, 1, 1)
    score_grad = (weights * (prob_grad - row_dots)).astype(jnp.bfloat16)
    dq_ref[...] = (contract(score_grad, all_keys, 0, 0) * scaling).astype(jnp.bfloat16)
    key_terms = jnp.dot(score_grad, query, preferred_element_type=jnp.float32) * scaling
    value_terms = jnp.dot(rounded, grad, preferred_element_type=jnp.float32)
    coarse_ref[:, :HEAD_DIM] = key_terms[fine:]
    coarse_ref[:, HEAD_DIM:] = value_terms[fine:]
    for j in range(SEL):
        place = place_ref[j]
        rows = slice(j * TILE, (j + 1) * TILE)
        for side, ref in enumerate((dnear_ref, dfar_ref)):
            start = pl.multiple_of((place % half) * TILE, TILE)

            @pl.when(place // half == side)
            def _():
                ref[pl.ds(start, TILE), :HEAD_DIM] = key_terms[rows].astype(jnp.bfloat16)
                ref[pl.ds(start, TILE), HEAD_DIM:] = value_terms[rows].astype(jnp.bfloat16)


def attend_heads(place, queries, grads_out, near, far, mean, first, heads):
    height = queries.shape[0]
    half = near.shape[0]
    pools = mean.shape[0]
    width = near.shape[1]
    count = pools + SEL * TILE
    at_head = lambda h, place: (0, h)
    in_head = lambda h, place: (0, first + h)
    return pl.pallas_call(
        head_kernel,
        grid_spec=pltpu.PrefetchScalarGridSpec(
            num_scalar_prefetch=1,
            grid=(heads,),
            in_specs=[
                pl.BlockSpec((height, HEAD_DIM), in_head),
                pl.BlockSpec((height, HEAD_DIM), in_head),
                pl.BlockSpec((half, 2 * HEAD_DIM), at_head),
                pl.BlockSpec((half, 2 * HEAD_DIM), at_head),
                pl.BlockSpec(mean.shape, lambda h, place: (0, 0)),
            ],
            out_specs=[
                pl.BlockSpec((height, HEAD_DIM), at_head),
                pl.BlockSpec((height, HEAD_DIM), at_head),
                pl.BlockSpec((half, 2 * HEAD_DIM), at_head),
                pl.BlockSpec((half, 2 * HEAD_DIM), at_head),
                pl.BlockSpec((pools, 2 * HEAD_DIM), at_head),
            ],
            scratch_shapes=[
                pltpu.VMEM((count, HEAD_DIM), jnp.bfloat16),
                pltpu.VMEM((count, HEAD_DIM), jnp.bfloat16),
            ],
        ),
        out_shape=[
            jax.ShapeDtypeStruct((height, heads * HEAD_DIM), jnp.bfloat16),
            jax.ShapeDtypeStruct((height, heads * HEAD_DIM), jnp.bfloat16),
            jax.ShapeDtypeStruct((half, width), jnp.bfloat16),
            jax.ShapeDtypeStruct((half, width), jnp.bfloat16),
            jax.ShapeDtypeStruct((pools, width), jnp.float32),
        ],
        cost_estimate=pl.CostEstimate(
            flops=heads * 12 * height * count * HEAD_DIM,
            bytes_accessed=16 * half * width,
            transcendentals=heads * height * count,
        ),
    )(place, queries, grads_out, near, far, mean)


def add(*terms):
    total = terms[0].astype(jnp.float32)
    for term in terms[1:]:
        total = total + term.astype(jnp.float32)
    return total.astype(jnp.bfloat16)


def dense_shards(query_rows, key_rows, value_rows, out_grad, selected):
    height, columns = query_rows.shape
    devices = lax.axis_size("ctx")
    ring = devices // (CORES * PAIR)
    me = lax.axis_index("ctx")

    def table(change):
        pairs = []
        for index in range(devices):
            z, x, core = index // (CORES * PAIR), index // CORES % PAIR, index % CORES
            z, x, core = change(z, x, core)
            pairs.append((index, (z % ring * PAIR + x) * CORES + core))
        return pairs

    across_core = table(lambda z, x, core: (z, x, 1 - core))
    across_x = table(lambda z, x, core: (z, 1 - x, core))
    upward = table(lambda z, x, core: (z + 1, x, core))
    downward = table(lambda z, x, core: (z - 1, x, core))
    move = lambda array, pairs: lax.ppermute(array, "ctx", pairs)

    def place_of(tile):
        step = (tile // (CORES * PAIR) - me // (CORES * PAIR)) % ring
        side = (tile // CORES + me // CORES) % PAIR
        other = (tile + me) % CORES
        return (other * ring + step) * PAIR + side

    place = place_of(selected[me]).astype(jnp.int32)
    tile_place = place_of(jnp.arange(devices, dtype=jnp.int32))
    per_tile = TILE // POOL
    starts = (tile_place[:, None] * per_tile + jnp.arange(per_tile)[None, :]).reshape(-1, 1)
    mean = (jnp.arange(devices * TILE)[None, :] // POOL == starts).astype(jnp.bfloat16)
    heads = HEADS // CHUNKS
    cut = heads * HEAD_DIM
    middle = TILE // 2

    def gather(chunk):
        span = slice(chunk * cut, (chunk + 1) * cut)
        own = jnp.stack(
            [
                key_rows[:, span].reshape(height, heads, HEAD_DIM),
                value_rows[:, span].reshape(height, heads, HEAD_DIM),
            ],
            axis=2,
        ).reshape(height, 2 * cut)
        side = move(own, across_x)
        below, above = move(own, upward), move(own, downward)
        below_side, above_side = move(side, upward), move(side, downward)
        far = jnp.concatenate(
            [move(below[:middle], upward), move(above[middle:], downward)], axis=0
        )
        far_side = move(far, across_x)
        near = jnp.concatenate(
            [own, side, above, above_side, far, far_side, below, below_side], axis=0
        )
        return near, move(near, across_core)

    def scatter(near, far):
        got = move(far, across_core)
        tile = lambda step, side: slice((step * PAIR + side) * TILE, (step * PAIR + side + 1) * TILE)
        part = lambda step, side: (near[tile(step, side)], got[tile(step, side)])
        crossed = move(add(*part(2, 1)), across_x)
        second = add(*part(2, 0), crossed)
        low = move(second[:middle], upward)
        high = move(second[middle:], downward)
        rise_near, rise_got = part(1, 0)
        fall_near, fall_got = part(3, 0)
        rise = jnp.concatenate(
            [
                add(rise_near[:middle], rise_got[:middle], low),
                add(rise_near[middle:], rise_got[middle:]),
            ],
            axis=0,
        )
        fall = jnp.concatenate(
            [
                add(fall_near[:middle], fall_got[:middle]),
                add(fall_near[middle:], fall_got[middle:], high),
            ],
            axis=0,
        )
        from_below_side = move(add(*part(1, 1)), upward)
        from_above_side = move(add(*part(3, 1)), downward)
        from_below = move(rise, upward)
        from_above = move(fall, downward)
        last = move(add(*part(0, 1), from_below_side, from_above_side), across_x)
        return add(*part(0, 0), from_below, from_above, last)

    gathered = [gather(chunk) for chunk in range(CHUNKS)]
    outs, queries, keys, values, coarse_keys, coarse_values = [], [], [], [], [], []
    for chunk, (near, far) in enumerate(gathered):
        out_rows, query_grad, dnear, dfar, coarse = attend_heads(
            place, query_rows, out_grad, near, far, mean, chunk * heads, heads
        )
        own_coarse = lax.psum_scatter(coarse, "ctx", scatter_dimension=0, tiled=True)
        fine = scatter(dnear, dfar)
        split_fine = fine.reshape(height, heads, 2, HEAD_DIM)
        split_coarse = own_coarse.reshape(-1, heads, 2, HEAD_DIM)
        sums = split_fine.astype(jnp.float32) + jnp.repeat(split_coarse, POOL, axis=0) / POOL
        sums = sums.astype(jnp.bfloat16)
        outs.append(out_rows)
        queries.append(query_grad)
        keys.append(sums[:, :, 0].reshape(height, cut))
        values.append(sums[:, :, 1].reshape(height, cut))
        coarse_keys.append(split_coarse[:, :, 0].reshape(-1, cut))
        coarse_values.append(split_coarse[:, :, 1].reshape(-1, cut))
    return tuple(
        jnp.concatenate(parts, axis=1)
        for parts in (outs, queries, keys, values, coarse_keys, coarse_values)
    )


def shards(query_rows, key_rows, value_rows, out_grad, selected):
    devices = lax.axis_size("ctx")
    few = devices <= PAIR * SEL and devices == 4 * CORES * PAIR
    whole_tile = query_rows.shape[0] == TILE
    chosen = dense_shards if few and whole_tile else listed_shards
    return chosen(query_rows, key_rows, value_rows, out_grad, selected)


def solution(mesh):
    in_specs = (
        P(("groups", "ctx"), None),
        P(("groups", "ctx"), None),
        P(("groups", "ctx"), None),
        P(("groups", "ctx"), None),
        P("groups", None),
    )
    out_specs = (
        P(("groups", "ctx"), None),
        P(("groups", "ctx"), None),
        P(("groups", "ctx"), None),
        P(("groups", "ctx"), None),
        P(("groups", "ctx"), None),
        P(("groups", "ctx"), None),
    )
    return jax.shard_map(shards, mesh=mesh, in_specs=in_specs, out_specs=out_specs, check_vma=False)
```

```python
import jax
import jax.numpy as jnp
from jax import lax
from jax.experimental import pallas as pl
from jax.experimental.pallas import tpu as pltpu
from jax.sharding import PartitionSpec as P


HEADS = 20
HEAD_DIM = 128
TILE = 128
POOL = 64
SEL = 8
CHUNKS = 4
SLOT = TILE + 16
CORES = 2
PAIR = 2


def pooled(rows):
    return jnp.mean(rows.astype(jnp.float32).reshape(-1, POOL, rows.shape[1]), axis=1).astype(
        jnp.bfloat16
    )


def contract(left, right, left_dim, right_dim):
    return lax.dot_general(
        left, right, (((left_dim,), (right_dim,)), ((), ())), preferred_element_type=jnp.float32
    )


def attend(queries, grads_out, keys_all, values_all):
    scaling = HEAD_DIM ** (-0.5)
    out_parts, query_parts, key_parts, value_parts = ([], [], [], [])
    for head in range(HEADS):
        lower = head * HEAD_DIM
        upper = lower + HEAD_DIM
        head_query = queries[:, lower:upper]
        head_grad = grads_out[:, lower:upper]
        head_key = keys_all[:, lower:upper]
        head_value = values_all[:, lower:upper]
        scores = contract(head_query, head_key, 1, 1) * scaling
        summit = jnp.max(scores, axis=-1, keepdims=True)
        raised = jnp.exp(scores - summit)
        weights = raised / jnp.sum(raised, axis=-1, keepdims=True)
        rounded = weights.astype(jnp.bfloat16)
        out_rows = jnp.dot(rounded, head_value, preferred_element_type=jnp.float32).astype(
            jnp.bfloat16
        )
        row_dots = jnp.sum(
            head_grad.astype(jnp.float32) * out_rows.astype(jnp.float32), axis=-1, keepdims=True
        )
        prob_grad = contract(head_grad, head_value, 1, 1)
        score_grad = (weights * (prob_grad - row_dots)).astype(jnp.bfloat16)
        query_grad = jnp.dot(score_grad, head_key, preferred_element_type=jnp.float32) * scaling
        key_terms = contract(score_grad, head_query, 0, 0) * scaling
        value_terms = contract(rounded, head_grad, 0, 0)
        out_parts.append(out_rows)
        query_parts.append(query_grad.astype(jnp.bfloat16))
        key_parts.append(key_terms)
        value_parts.append(value_terms)
    return (
        jnp.concatenate(out_parts, axis=1),
        jnp.concatenate(query_parts, axis=1),
        jnp.concatenate(key_parts, axis=1),
        jnp.concatenate(value_parts, axis=1),
    )


def package(tiles_in, pooled_in, devices, spread):
    tiles_here, tile_len, columns = tiles_in.shape
    per_tile = tile_len // POOL
    split_rows = tiles_in.reshape(tiles_here, devices, spread, columns)
    copies = jnp.broadcast_to(
        pooled_in.reshape(tiles_here, 1, per_tile, columns),
        (tiles_here, devices, per_tile, columns),
    )
    return jnp.concatenate([split_rows, copies], axis=2).reshape(
        tiles_here, devices * (spread + per_tile), columns
    )


def listed_shards(query_rows, key_rows, value_rows, out_grad, selected):
    height, columns = query_rows.shape
    devices = lax.axis_size("ctx")
    tiles_here = height // TILE
    spread = TILE // devices
    own_keys = pooled(key_rows)
    own_values = pooled(value_rows)
    key_tiles = key_rows.reshape(tiles_here, TILE, columns)
    value_tiles = value_rows.reshape(tiles_here, TILE, columns)
    joined_keys, joined_values = (
        lax.all_to_all(
            package(key_tiles, own_keys, devices, spread),
            "ctx",
            split_axis=1,
            concat_axis=0,
            tiled=True,
        ),
        lax.all_to_all(
            package(value_tiles, own_values, devices, spread),
            "ctx",
            split_axis=1,
            concat_axis=0,
            tiled=True,
        ),
    )
    held_keys = joined_keys[:, :spread]
    held_values = joined_values[:, :spread]
    pool_keys = joined_keys[:, spread:].reshape(-1, columns)
    pool_values = joined_values[:, spread:].reshape(-1, columns)
    comp_count = pool_keys.shape[0]
    got_keys, got_values = (
        lax.all_to_all(held_keys[selected], "ctx", split_axis=0, concat_axis=2, tiled=True),
        lax.all_to_all(held_values[selected], "ctx", split_axis=0, concat_axis=2, tiled=True),
    )
    fine_keys = got_keys.reshape(tiles_here, SEL * TILE, columns)
    fine_values = got_values.reshape(tiles_here, SEL * TILE, columns)
    out_tiles, query_tiles, key_listed, value_listed = ([], [], [], [])
    keys_all = jnp.concatenate([pool_keys, fine_keys[0]], axis=0)
    values_all = jnp.concatenate([pool_values, fine_values[0]], axis=0)
    out_rows, query_grad, key_terms, value_terms = attend(
        query_rows, out_grad, keys_all, values_all
    )
    out_tiles.append(out_rows)
    query_tiles.append(query_grad)
    coarse_keys = key_terms[:comp_count]
    coarse_values = value_terms[:comp_count]
    key_listed.append(key_terms[comp_count:].astype(jnp.bfloat16))
    value_listed.append(value_terms[comp_count:].astype(jnp.bfloat16))
    own_coarse_keys, own_coarse_values = (
        lax.psum_scatter(coarse_keys, "ctx", scatter_dimension=0, tiled=True),
        lax.psum_scatter(coarse_values, "ctx", scatter_dimension=0, tiled=True),
    )
    listed_keys = jnp.stack(key_listed).reshape(tiles_here * SEL, devices, spread, columns)
    listed_values = jnp.stack(value_listed).reshape(tiles_here * SEL, devices, spread, columns)
    back_keys, back_values = (
        lax.all_to_all(listed_keys, "ctx", split_axis=1, concat_axis=0, tiled=True),
        lax.all_to_all(listed_values, "ctx", split_axis=1, concat_axis=0, tiled=True),
    )
    tile_ids = jnp.arange(selected.shape[0], dtype=jnp.int32)[:, None]
    member = (selected.reshape(1, -1) == tile_ids).astype(jnp.bfloat16)
    entries = member.shape[1]
    sum_keys = jnp.dot(
        member, back_keys.reshape(entries, spread * columns), preferred_element_type=jnp.float32
    )
    sum_values = jnp.dot(
        member, back_values.reshape(entries, spread * columns), preferred_element_type=jnp.float32
    )
    held_key_grad = sum_keys.astype(jnp.bfloat16).reshape(devices, tiles_here, spread, columns)
    held_value_grad = sum_values.astype(jnp.bfloat16).reshape(devices, tiles_here, spread, columns)
    owned_keys, owned_values = (
        lax.all_to_all(held_key_grad, "ctx", split_axis=0, concat_axis=2, tiled=True),
        lax.all_to_all(held_value_grad, "ctx", split_axis=0, concat_axis=2, tiled=True),
    )
    grad_key = (
        owned_keys.reshape(height, columns).astype(jnp.float32)
        + jnp.repeat(own_coarse_keys, POOL, axis=0) / POOL
    ).astype(jnp.bfloat16)
    grad_value = (
        owned_values.reshape(height, columns).astype(jnp.float32)
        + jnp.repeat(own_coarse_values, POOL, axis=0) / POOL
    ).astype(jnp.bfloat16)
    attended = out_tiles[0]
    grad_query = query_tiles[0]
    return (attended, grad_query, grad_key, grad_value, own_coarse_keys, own_coarse_values)


def head_kernel(place_ref, query_ref, grad_ref, near_ref, far_ref, mean_ref, out_ref, dq_ref,
                dnear_ref, dfar_ref, keys, values):
    half = near_ref.shape[0] // TILE
    fine = SEL * TILE
    means = (
        jnp.dot(mean_ref[:, : half * TILE], near_ref[...], preferred_element_type=jnp.float32)
        + jnp.dot(mean_ref[:, half * TILE :], far_ref[...], preferred_element_type=jnp.float32)
    ) * (1.0 / POOL)
    keys[fine:, :] = means[:, :HEAD_DIM].astype(jnp.bfloat16)
    values[fine:, :] = means[:, HEAD_DIM:].astype(jnp.bfloat16)
    dnear_ref[...] = jnp.zeros_like(dnear_ref)
    dfar_ref[...] = jnp.zeros_like(dfar_ref)
    for j in range(SEL):
        place = place_ref[j]
        rows = slice(j * TILE, (j + 1) * TILE)
        for side, ref in enumerate((near_ref, far_ref)):
            start = pl.multiple_of((place % half) * TILE, TILE)

            @pl.when(place // half == side)
            def _():
                keys[rows, :] = ref[pl.ds(start, TILE), :HEAD_DIM]
                values[rows, :] = ref[pl.ds(start, TILE), HEAD_DIM:]

    scaling = HEAD_DIM ** (-0.5)
    query = query_ref[...]
    grad = grad_ref[...]
    all_keys = keys[...]
    all_values = values[...]
    scores = contract(all_keys, query, 1, 1)
    summit = jnp.max(scores, axis=0, keepdims=True)
    raised = jnp.exp((scores - summit) * scaling)
    weights = raised * (1.0 / jnp.sum(raised, axis=0, keepdims=True))
    rounded = weights.astype(jnp.bfloat16)
    out_rows = contract(rounded, all_values, 0, 0).astype(jnp.bfloat16)
    out_ref[...] = out_rows
    products = grad.astype(jnp.float32) * out_rows.astype(jnp.float32)
    row_dots = jnp.sum(products.T, axis=0, keepdims=True)
    prob_grad = contract(all_values, grad, 1, 1)
    score_grad = (weights * (prob_grad - row_dots)).astype(jnp.bfloat16)
    dq_ref[...] = (contract(score_grad, all_keys, 0, 0) * scaling).astype(jnp.bfloat16)
    key_terms = jnp.dot(score_grad, query, preferred_element_type=jnp.float32) * scaling
    value_terms = jnp.dot(rounded, grad, preferred_element_type=jnp.float32)
    per_tile = TILE // POOL
    for tile in range(2 * half):
        ref = dnear_ref if tile < half else dfar_ref
        rows = slice(fine + tile * per_tile, fine + (tile + 1) * per_tile)
        start = tile % half * SLOT + TILE
        ref[start : start + per_tile, :HEAD_DIM] = key_terms[rows].astype(jnp.bfloat16)
        ref[start : start + per_tile, HEAD_DIM:] = value_terms[rows].astype(jnp.bfloat16)
    for j in range(SEL):
        place = place_ref[j]
        rows = slice(j * TILE, (j + 1) * TILE)
        for side, ref in enumerate((dnear_ref, dfar_ref)):
            start = pl.multiple_of((place % half) * SLOT, 16)

            @pl.when(place // half == side)
            def _():
                ref[pl.ds(start, TILE), :HEAD_DIM] = key_terms[rows].astype(jnp.bfloat16)
                ref[pl.ds(start, TILE), HEAD_DIM:] = value_terms[rows].astype(jnp.bfloat16)


def attend_heads(place, queries, grads_out, near, far, mean, first, heads):
    height = queries.shape[0]
    half = near.shape[0]
    slots = half // TILE * SLOT
    pools = mean.shape[0]
    width = near.shape[1]
    count = pools + SEL * TILE
    at_head = lambda h, place: (0, h)
    in_head = lambda h, place: (0, first + h)
    return pl.pallas_call(
        head_kernel,
        grid_spec=pltpu.PrefetchScalarGridSpec(
            num_scalar_prefetch=1,
            grid=(heads,),
            in_specs=[
                pl.BlockSpec((height, HEAD_DIM), in_head),
                pl.BlockSpec((height, HEAD_DIM), in_head),
                pl.BlockSpec((half, 2 * HEAD_DIM), at_head),
                pl.BlockSpec((half, 2 * HEAD_DIM), at_head),
                pl.BlockSpec(mean.shape, lambda h, place: (0, 0)),
            ],
            out_specs=[
                pl.BlockSpec((height, HEAD_DIM), at_head),
                pl.BlockSpec((height, HEAD_DIM), at_head),
                pl.BlockSpec((slots, 2 * HEAD_DIM), at_head),
                pl.BlockSpec((slots, 2 * HEAD_DIM), at_head),
            ],
            scratch_shapes=[
                pltpu.VMEM((count, HEAD_DIM), jnp.bfloat16),
                pltpu.VMEM((count, HEAD_DIM), jnp.bfloat16),
            ],
        ),
        out_shape=[
            jax.ShapeDtypeStruct((height, heads * HEAD_DIM), jnp.bfloat16),
            jax.ShapeDtypeStruct((height, heads * HEAD_DIM), jnp.bfloat16),
            jax.ShapeDtypeStruct((slots, width), jnp.bfloat16),
            jax.ShapeDtypeStruct((slots, width), jnp.bfloat16),
        ],
        cost_estimate=pl.CostEstimate(
            flops=heads * 12 * height * count * HEAD_DIM,
            bytes_accessed=16 * half * width,
            transcendentals=heads * height * count,
        ),
    )(place, queries, grads_out, near, far, mean)


def add(*terms):
    total = terms[0].astype(jnp.float32)
    for term in terms[1:]:
        total = total + term.astype(jnp.float32)
    return total.astype(jnp.bfloat16)


def dense_shards(query_rows, key_rows, value_rows, out_grad, selected):
    height, _ = query_rows.shape
    devices = lax.axis_size("ctx")
    ring = devices // (CORES * PAIR)
    me = lax.axis_index("ctx")

    def table(change):
        pairs = []
        for index in range(devices):
            z, x, core = index // (CORES * PAIR), index // CORES % PAIR, index % CORES
            z, x, core = change(z, x, core)
            pairs.append((index, (z % ring * PAIR + x) * CORES + core))
        return pairs

    across_core = table(lambda z, x, core: (z, x, 1 - core))
    across_x = table(lambda z, x, core: (z, 1 - x, core))
    upward = table(lambda z, x, core: (z + 1, x, core))
    downward = table(lambda z, x, core: (z - 1, x, core))
    move = lambda array, pairs: lax.ppermute(array, "ctx", pairs)

    def place_of(tile):
        step = (tile // (CORES * PAIR) - me // (CORES * PAIR)) % ring
        side = (tile // CORES + me // CORES) % PAIR
        other = (tile + me) % CORES
        return (other * ring + step) * PAIR + side

    place = place_of(selected[me]).astype(jnp.int32)
    pools = devices * TILE // POOL
    mean = (jnp.arange(devices * TILE)[None, :] // POOL == jnp.arange(pools)[:, None]).astype(
        jnp.bfloat16
    )
    heads = HEADS // CHUNKS
    cut = heads * HEAD_DIM
    middle = TILE // 2

    def gather(chunk):
        span = slice(chunk * cut, (chunk + 1) * cut)
        own = jnp.stack(
            [
                key_rows[:, span].reshape(height, heads, HEAD_DIM),
                value_rows[:, span].reshape(height, heads, HEAD_DIM),
            ],
            axis=2,
        ).reshape(height, 2 * cut)
        side = move(own, across_x)
        below, above = move(own, upward), move(own, downward)
        below_side, above_side = move(side, upward), move(side, downward)
        far = jnp.concatenate(
            [move(below[:middle], upward), move(above[middle:], downward)], axis=0
        )
        far_side = move(far, across_x)
        near = jnp.concatenate(
            [own, side, above, above_side, far, far_side, below, below_side], axis=0
        )
        return near, move(near, across_core)

    def scatter(near, far):
        got = move(far, across_core)
        tile = lambda step, side: slice((step * PAIR + side) * SLOT, (step * PAIR + side + 1) * SLOT)
        part = lambda step, side: (near[tile(step, side)], got[tile(step, side)])
        center = SLOT // 32 * 16
        crossed = move(add(*part(2, 1)), across_x)
        second = add(*part(2, 0), crossed)
        low = move(second[:center], upward)
        high = move(second[center:], downward)
        rise_near, rise_got = part(1, 0)
        fall_near, fall_got = part(3, 0)
        rise = jnp.concatenate(
            [
                add(rise_near[:center], rise_got[:center], low),
                add(rise_near[center:], rise_got[center:]),
            ],
            axis=0,
        )
        fall = jnp.concatenate(
            [
                add(fall_near[:center], fall_got[:center]),
                add(fall_near[center:], fall_got[center:], high),
            ],
            axis=0,
        )
        from_below_side = move(add(*part(1, 1)), upward)
        from_above_side = move(add(*part(3, 1)), downward)
        from_below = move(rise, upward)
        from_above = move(fall, downward)
        last = move(add(*part(0, 1), from_below_side, from_above_side), across_x)
        return add(*part(0, 0), from_below, from_above, last)

    gathered = [gather(chunk) for chunk in range(CHUNKS)]
    outs, queries, keys, values, coarse_keys, coarse_values = [], [], [], [], [], []
    for chunk, (near, far) in enumerate(gathered):
        out_rows, query_grad, dnear, dfar = attend_heads(
            place, query_rows, out_grad, near, far, mean, chunk * heads, heads
        )
        total = scatter(dnear, dfar)
        split_fine = total[:height].reshape(height, heads, 2, HEAD_DIM)
        split_coarse = total[height : height + TILE // POOL].astype(jnp.float32)
        split_coarse = split_coarse.reshape(-1, heads, 2, HEAD_DIM)
        sums = split_fine.astype(jnp.float32) + jnp.repeat(split_coarse, POOL, axis=0) / POOL
        sums = sums.astype(jnp.bfloat16)
        outs.append(out_rows)
        queries.append(query_grad)
        keys.append(sums[:, :, 0].reshape(height, cut))
        values.append(sums[:, :, 1].reshape(height, cut))
        coarse_keys.append(split_coarse[:, :, 0].reshape(-1, cut))
        coarse_values.append(split_coarse[:, :, 1].reshape(-1, cut))
    return tuple(
        jnp.concatenate(parts, axis=1)
        for parts in (outs, queries, keys, values, coarse_keys, coarse_values)
    )


def shards(query_rows, key_rows, value_rows, out_grad, selected):
    devices = lax.axis_size("ctx")
    few = devices <= PAIR * SEL and devices == 4 * CORES * PAIR
    whole_tile = query_rows.shape[0] == TILE
    chosen = dense_shards if few and whole_tile else listed_shards
    if chosen is listed_shards:
        return listed_shards(query_rows, key_rows, value_rows, out_grad, selected)
    return dense_shards(query_rows, key_rows, value_rows, out_grad, selected)


def solution(mesh):
    in_specs = (
        P(("groups", "ctx"), None),
        P(("groups", "ctx"), None),
        P(("groups", "ctx"), None),
        P(("groups", "ctx"), None),
        P("groups", None),
    )
    out_specs = (
        P(("groups", "ctx"), None),
        P(("groups", "ctx"), None),
        P(("groups", "ctx"), None),
        P(("groups", "ctx"), None),
        P(("groups", "ctx"), None),
        P(("groups", "ctx"), None),
    )
    return jax.shard_map(shards, mesh=mesh, in_specs=in_specs, out_specs=out_specs, check_vma=False)
```
